32 devices in a mesh: grp: 8 (over z, x), seq: 4 (over y, core).
Axes of the slice: x: 2, y: 2, z: 4, core: 2. Of those that a mesh axis runs over, the one named last changes fastest.
Arguments:
- inputs: bfloat16 [2, 8, 512, 1536], P(None, 'grp', 'seq'), may hold values from -6 to 6
- cont_lengths: int32 [2, 8, 2], P(None, 'grp'), may hold values from 1 to 256, 448 in all within a row
- w_query: bfloat16 [1536, 1536], P(('grp', 'seq')), may hold values from -0.15625 to 0.15625
- key_projection: bfloat16 [1536, 768], P(('grp', 'seq')), may hold values from -0.15625 to 0.15625
- value_projection: bfloat16 [1536, 768], P(('grp', 'seq')), may hold values from -0.15625 to 0.15625
- w_out: bfloat16 [1536, 1536], P(None, ('grp', 'seq')), may hold values from -1.75 to 1.75
- attn_gain: bfloat16 [1536], P(('grp', 'seq')), may hold values from 0.25 to 1.75
- w_gate: bfloat16 [1536, 4096], P(('grp', 'seq')), may hold values from -0.15625 to 0.15625
- w_up: bfloat16 [1536, 4096], P(('grp', 'seq')), may hold values from -0.15625 to 0.15625
- w_down: bfloat16 [4096, 1536], P(('grp', 'seq')), may hold values from -0.09375 to 0.09375
- mlp_gain: bfloat16 [1536], P(('grp', 'seq')), may hold values from 0.25 to 1.75
- cotangent: bfloat16 [2, 8, 512, 1536], P(None, 'grp', 'seq'), may hold values from -6 to 6
Outputs:
- outputs: bfloat16 [2, 8, 512, 1536], P(None, 'grp', 'seq')
- grad_inputs: float32 [2, 8, 512, 1536], P(None, 'grp', 'seq')
- grad_query: float32 [1536, 1536], P(('grp', 'seq'))
- grad_key: float32 [1536, 768], P(('grp', 'seq'))
- grad_value: float32 [1536, 768], P(('grp', 'seq'))
- grad_out: float32 [1536, 1536], P(None, ('grp', 'seq'))
- grad_attn_gain: float32 [1536], P(('grp', 'seq'))
- grad_gate: float32 [1536, 4096], P(('grp', 'seq'))
- grad_up: float32 [1536, 4096], P(('grp', 'seq'))
- grad_down: float32 [4096, 1536], P(('grp', 'seq'))
- grad_mlp_gain: float32 [1536], P(('grp', 'seq'))
The draws below stay inside these ranges and needn't reach their ends.
Inputs may be any that keep to these rules, and one draw needn't show every extreme that they name: `cont_lengths`: each group's 2 continuation lengths sum to 448.
All inputs are finite; a program needn't handle non-finite values.
Results may differ from the reference program's by a relative error of at most 0.017.
Values may be sent and summed in bfloat16 or wider, within the bound.
A program may use at most 320 MiB of HBM per device.

```python
import math
import jax
import jax.numpy as jnp
import numpy as np
from jax import lax

MODEL_WIDTH = 1536
QUERY_HEADS = 16
KEY_VALUE_HEADS = 8
HEAD_SIZE = 96
FF = 4096
ROWS_DEV = 128
MB = 2
CONT_LEN = 256
GROUP_ROWS = 512
CONTS = 2
CONT_TOTAL = 448
PROMPT = 64
N_GRP = 8
N_SEQ = 4


def strengthened(drawn, own_key, source, target, parts, factor):
    def block_of(axis_at):
        return (jnp.arange(drawn.shape[axis_at]) // (drawn.shape[axis_at] // parts)).reshape((-1,) + (1,) * (drawn.ndim - 1 - axis_at))

    near = jax.random.permutation(own_key, parts)[block_of(target)]
    second = (block_of(target) + parts // 2) % parts
    return jnp.where((block_of(source) == near) | (block_of(source) == second), factor * drawn, drawn)


def block_levels(rng, dims, pieces, smallest, top_value):
    level, own = 1.0, jax.random.fold_in(rng, 6)
    for axis_at, parts in pieces:
        draws = jnp.exp(jax.random.uniform(jax.random.fold_in(own, axis_at), (parts,), jnp.float32, smallest / len(pieces), top_value / len(pieces)))
        level = level * jnp.repeat(draws, dims[axis_at] // parts).reshape([-1 if axis == axis_at else 1 for axis in range(len(dims))])
    return level


def split_up(count, total, limit, lean):
    weights = [(1 << 20) // math.isqrt(grade ** lean) + 1 for grade in range(2, count + 1)]
    spare, given = total - limit - (count - 1), [1] * (count - 1)
    while spare > 0:
        candidates = [i for i in range(count - 1) if given[i] < limit]
        whole, remaining = sum([weights[i] for i in candidates]), spare
        for i in candidates:
            more = min(limit - given[i], max(1, remaining * weights[i] // whole), spare)
            given[i] = given[i] + more
            spare = spare - more
    return np.array([limit] + given)


def uneven_parts(own_key, amount, total, reach, lean):
    if amount == 2:
        one = jax.random.randint(own_key, (), max(1, total - reach), min(reach, total - 1) + 1)
        return jnp.stack([one, total - one])
    sizes = jnp.asarray(split_up(amount, total, reach, lean), jnp.int32)
    twos = (amount - 1) // 2
    source_of, receiver = sizes[1:1 + 2 * twos:2], sizes[2:2 + 2 * twos:2]
    room = jnp.minimum(source_of - 1, reach - receiver)
    passed = jax.random.randint(jax.random.fold_in(own_key, 1), (twos,), 0, 1 << 20) % (room + 1)
    sizes = sizes.at[1:1 + 2 * twos:2].set(source_of - passed).at[2:2 + 2 * twos:2].set(receiver + passed)
    return sizes[jax.random.permutation(jax.random.fold_in(own_key, 2), amount)]


def bell_draw(stream_key, extent, scale, reach, pieces=(), held_as=jnp.bfloat16):
    entries = scale * jax.random.normal(stream_key, extent, jnp.float32)
    if pieces:
        entries = entries * block_levels(stream_key, extent, pieces, -0.22, 0.18)
    return jnp.clip(entries, -reach, reach).astype(held_as)


def gaussian_with(own_key, dims, spread, bound, split, heavy, held_as=jnp.bfloat16):
    values = spread * jax.random.normal(own_key, dims, jnp.float32)
    if split:
        values = values * block_levels(own_key, dims, split, -0.22, 0.18)
    return jnp.clip(strengthened(values, jax.random.fold_in(own_key, 3), *heavy), -bound, bound).astype(held_as)


def setup_inputs(seed: int = 0) -> dict:
    key_of = jax.random.split(jax.random.key(seed), 13)
    return {
        "inputs": bell_draw(key_of[0], (MB, N_GRP, GROUP_ROWS, MODEL_WIDTH), 1.0, 6.0, ((1, 8), (2, 4))),
        "cont_lengths": jax.vmap(lambda own: uneven_parts(own, CONTS, CONT_TOTAL, CONT_LEN, 2))(jax.random.split(key_of[1], MB * N_GRP)).reshape((MB, N_GRP, CONTS)).astype(jnp.int32),
        "w_query": bell_draw(key_of[2], (MODEL_WIDTH, QUERY_HEADS * HEAD_SIZE), MODEL_WIDTH ** -0.5, 0.15625, ((0, 32),)),
        "key_projection": bell_draw(key_of[3], (MODEL_WIDTH, KEY_VALUE_HEADS * HEAD_SIZE), MODEL_WIDTH ** -0.5, 0.15625, ((0, 32),)),
        "value_projection": bell_draw(key_of[4], (MODEL_WIDTH, KEY_VALUE_HEADS * HEAD_SIZE), MODEL_WIDTH ** -0.5, 0.15625, ((0, 32),)),
        "w_out": bell_draw(key_of[5], (QUERY_HEADS * HEAD_SIZE, MODEL_WIDTH), (max(2, 4 * QUERY_HEADS * HEAD_SIZE // GROUP_ROWS)) ** -0.5, 1.75, ((1, 32),)),
        "attn_gain": jnp.clip(1.0 + 0.15 * jax.random.normal(key_of[6], (MODEL_WIDTH,), jnp.float32), 0.25, 1.75).astype(jnp.bfloat16),
        "w_gate": bell_draw(key_of[7], (MODEL_WIDTH, FF), MODEL_WIDTH ** -0.5, 0.15625, ((0, 32),)),
        "w_up": bell_draw(key_of[8], (MODEL_WIDTH, FF), MODEL_WIDTH ** -0.5, 0.15625, ((0, 32),)),
        "w_down": bell_draw(key_of[9], (FF, MODEL_WIDTH), FF ** -0.5, 0.09375, ((0, 32),)),
        "mlp_gain": jnp.clip(1.0 + 0.15 * jax.random.normal(key_of[10], (MODEL_WIDTH,), jnp.float32), 0.25, 1.75).astype(jnp.bfloat16),
        "cotangent": gaussian_with(key_of[11], (MB, N_GRP, GROUP_ROWS, MODEL_WIDTH), 1.0, 6.0, ((1, 8), (2, 4)), (2, 3, 4, 2.0)),
    }


EPSILON = 1e-05
ROPE_BASE = 100000.0
MASK_FILL = -1e+30
HIGHEST = lax.Precision.HIGHEST

@jax.custom_vjp
def reduced_precision(v):
    return lax.optimization_barrier(v.astype(jnp.bfloat16)).astype(jnp.float32)

@jax.custom_vjp
def low_back(v):
    return v

def low_keep(v):
    return (reduced_precision(v), None)

def low_pass(kept, grad):
    return (grad,)

def back_keep(v):
    return (v, None)

def back_low(kept, grad):
    return (reduced_precision(grad),)
reduced_precision.defvjp(low_keep, low_pass)
low_back.defvjp(back_keep, back_low)

def layout(lengths, rows_per_group, prompt_rows):
    row_ids = jnp.arange(rows_per_group, dtype=jnp.int32)
    cont_ends = (prompt_rows + jnp.cumsum(lengths)).astype(jnp.int32)
    cont_starts = (cont_ends - lengths).astype(jnp.int32)
    member = ((row_ids[:, None] >= cont_starts[None, :]) & (row_ids[:, None] < cont_ends[None, :])).astype(jnp.int32)
    labels = jnp.arange(1, lengths.shape[0] + 1, dtype=jnp.int32)
    segment = lax.optimization_barrier(jnp.sum(member * labels[None, :], axis=1)).astype(jnp.int32)
    offsets = lax.optimization_barrier(jnp.sum(member * cont_starts[None, :], axis=1)).astype(jnp.int32)
    position = jnp.where(segment > 0, prompt_rows + row_ids - offsets, row_ids).astype(jnp.int32)
    return (segment, position)

def rotation(position):
    half_dim = HEAD_SIZE // 2
    frequency = ROPE_BASE ** (-2.0 * jnp.arange(half_dim, dtype=jnp.float32) / HEAD_SIZE)
    angles = position.astype(jnp.float32)[:, None] * frequency[None, :]
    return (jnp.cos(angles), jnp.sin(angles))

def apply_rotary(head_values, cosine_lookup, sine_lookup):
    half_dim = head_values.shape[-1] // 2
    first_half = head_values[..., :half_dim]
    second_half = head_values[..., half_dim:]
    cos_wide = cosine_lookup[:, None, :]
    sin_wide = sine_lookup[:, None, :]
    return jnp.concatenate([first_half * cos_wide - second_half * sin_wide, second_half * cos_wide + first_half * sin_wide], axis=-1)

def rms_norm(row_values, gain):
    inverse = lax.rsqrt(lax.optimization_barrier(jnp.mean(row_values * row_values, axis=-1, keepdims=True)) + EPSILON)
    return row_values * inverse * gain

def matmul(left, right):
    return jnp.dot(left, right, precision=HIGHEST, preferred_element_type=jnp.float32)

def attend(query_rows, key_lookup, value_lookup, segment, position):
    head_repeat_factor = QUERY_HEADS // KEY_VALUE_HEADS
    grouped_queries = query_rows.reshape(GROUP_ROWS, KEY_VALUE_HEADS, head_repeat_factor, HEAD_SIZE)

    def block(row_start):
        query_part = lax.dynamic_slice_in_dim(grouped_queries, row_start, ROWS_DEV, 0)
        segment_part = lax.dynamic_slice_in_dim(segment, row_start, ROWS_DEV, 0)
        position_part = lax.dynamic_slice_in_dim(position, row_start, ROWS_DEV, 0)
        same_seq = (segment[None, :] == 0) | (segment[None, :] == segment_part[:, None])
        visible = same_seq & (position[None, :] <= position_part[:, None])
        scores = low_back(jnp.einsum('rgjd,kgd->gjrk', query_part, key_lookup, precision=HIGHEST))
        scores = jnp.where(visible[None, None], scores, MASK_FILL)
        probs = reduced_precision(jax.nn.softmax(scores, axis=-1))
        mixed_rows = jnp.einsum('gjrk,kgd->rgjd', probs, value_lookup, precision=HIGHEST)
        return mixed_rows.reshape(ROWS_DEV, QUERY_HEADS * HEAD_SIZE)
    row_starts = jnp.arange(N_SEQ, dtype=jnp.int32) * ROWS_DEV
    return lax.map(jax.checkpoint(block), row_starts).reshape(GROUP_ROWS, QUERY_HEADS * HEAD_SIZE)

def forward(inputs_float, weight_list, segment, position):
    query_weight, key_weight, value_weight, out_weight, attn_gain, gate_weight, up_weight, down_weight, mlp_gain = weight_list
    act_one = reduced_precision(rms_norm(inputs_float, attn_gain))
    query_pre = low_back(matmul(act_one, query_weight))
    key_unrotated = low_back(matmul(act_one, key_weight))
    value_projected = low_back(matmul(act_one, value_weight))
    cosine_lookup, sine_lookup = rotation(position)
    query_rows = reduced_precision(apply_rotary(query_pre.reshape(GROUP_ROWS, QUERY_HEADS, HEAD_SIZE), cosine_lookup, sine_lookup) * HEAD_SIZE ** (-0.5))
    key_lookup = reduced_precision(apply_rotary(key_unrotated.reshape(GROUP_ROWS, KEY_VALUE_HEADS, HEAD_SIZE), cosine_lookup, sine_lookup))
    value_lookup = reduced_precision(value_projected.reshape(GROUP_ROWS, KEY_VALUE_HEADS, HEAD_SIZE))
    attn_flat = attend(query_rows, key_lookup, value_lookup, segment, position)
    attn_low = reduced_precision(low_back(attn_flat))
    hidden = inputs_float + low_back(matmul(attn_low, out_weight))
    act_two = reduced_precision(rms_norm(hidden, mlp_gain))
    gate_pre = low_back(matmul(act_two, gate_weight))
    up_pre = low_back(matmul(act_two, up_weight))
    mixed_act = reduced_precision(jax.nn.silu(gate_pre) * up_pre)
    return hidden + low_back(matmul(mixed_act, down_weight))

def reference(inputs, cont_lengths, w_query, key_projection, value_projection, w_out, attn_gain, w_gate, w_up, w_down, mlp_gain, cotangent):
    weights = tuple((array.astype(jnp.float32) for array in (w_query, key_projection, value_projection, w_out, attn_gain, w_gate, w_up, w_down, mlp_gain)))
    group_count = MB * N_GRP
    input_groups = inputs.reshape(group_count, GROUP_ROWS, MODEL_WIDTH)
    length_groups = cont_lengths.reshape(group_count, CONTS)
    cot_groups = cotangent.reshape(group_count, GROUP_ROWS, MODEL_WIDTH)

    def one_group(running, group_item):
        rows_in, lengths, cot_rows = group_item
        segment, position = layout(lengths, GROUP_ROWS, PROMPT)

        def run(inputs_float, *weight_list):
            return forward(inputs_float, weight_list, segment, position)
        result, pull_back = jax.vjp(run, rows_in.astype(jnp.float32), *weights)
        grad_list = pull_back(cot_rows.astype(jnp.float32))
        new_running = tuple((running_sum + grad_part for running_sum, grad_part in zip(running, grad_list[1:])))
        return (new_running, (result.astype(jnp.bfloat16), grad_list[0]))
    start_sums = tuple((jnp.zeros(array.shape, jnp.float32) for array in weights))
    totals, (result_rows, grad_rows) = lax.scan(one_group, start_sums, (input_groups, length_groups, cot_groups))
    return (result_rows.reshape(MB, N_GRP, GROUP_ROWS, MODEL_WIDTH), grad_rows.reshape(MB, N_GRP, GROUP_ROWS, MODEL_WIDTH), totals[0], totals[1], totals[2], totals[3], totals[4], totals[5], totals[6], totals[7], totals[8])
```

```python
import jax
import jax.numpy as jnp
from jax import lax
from jax.sharding import Mesh
from jax.sharding import PartitionSpec as P

QUERY_HEADS = 16
KEY_VALUE_HEADS = 8
HEAD_SIZE = 96
CONT_MEAN = 224

EPSILON = 1e-05
ROPE_BASE = 100000.0
MASK_FILL = -1e30
CHIPS = ("grp", "row")
F32 = jnp.float32
BF16 = jnp.bfloat16


def layout(lengths, row_ids, prompt_rows):
    cont_ends = prompt_rows + jnp.cumsum(lengths)
    cont_starts = cont_ends - lengths
    member = (
        (row_ids[:, None] >= cont_starts[None, :]) & (row_ids[:, None] < cont_ends[None, :])
    ).astype(jnp.int32)
    labels = jnp.arange(1, lengths.shape[0] + 1, dtype=jnp.int32)
    segment = jnp.sum(member * labels[None, :], axis=1)
    offsets = jnp.sum(member * cont_starts[None, :], axis=1)
    position = jnp.where(segment > 0, prompt_rows + row_ids - offsets, row_ids)
    return (segment, position)


def rotation(position):
    half_dim = HEAD_SIZE // 2
    frequency = ROPE_BASE ** (-2.0 * jnp.arange(half_dim, dtype=F32) / HEAD_SIZE)
    angles = position.astype(F32)[..., None] * frequency
    return (jnp.cos(angles)[..., None, :], jnp.sin(angles)[..., None, :])


def rotate(head_values, cosine, sine):
    half_dim = HEAD_SIZE // 2
    first, second = head_values[..., :half_dim], head_values[..., half_dim:]
    return jnp.concatenate(
        [first * cosine - second * sine, second * cosine + first * sine], axis=-1
    )


def dot(left, right, left_dim, right_dim):
    return lax.dot_general(
        left, right, (((left_dim,), (right_dim,)), ((), ())), preferred_element_type=F32
    )


def swap(value):
    return lax.ppermute(value, "core", [(0, 1), (1, 0)])


def take_half(value, which):
    half = value.shape[1] // 2
    return lax.dynamic_slice_in_dim(value, which * half, half, 1)


def on_device(
    inputs,
    cont_lengths,
    w_query,
    key_projection,
    value_projection,
    w_out,
    attn_gain,
    w_gate,
    w_up,
    w_down,
    mlp_gain,
    cotangent,
):
    micros, _, rows_own, width = inputs.shape
    n_row = lax.axis_size("row")
    chips = lax.axis_size("grp") * n_row
    core = lax.axis_index("core")
    chip_row = lax.axis_index("row")
    rows_chip = 2 * rows_own
    rows_group = rows_chip * n_row
    rows = micros * rows_chip
    prompt_rows = rows_group - CONT_MEAN * cont_lengths.shape[2]
    repeat = QUERY_HEADS // KEY_VALUE_HEADS
    kv_heads = KEY_VALUE_HEADS // 2
    q_heads = QUERY_HEADS // 2
    q_cols, kv_cols = q_heads * HEAD_SIZE, kv_heads * HEAD_SIZE
    scale = HEAD_SIZE ** (-0.5)
    feats = w_query.shape[0]
    hidden_own = w_down.shape[0]
    ff_half = hidden_own * chips

    gain_one = attn_gain.astype(F32)[:, None]
    gain_two = mlp_gain.astype(F32)[:, None]

    def ff_part(value, which):
        parts = value.reshape(feats, chips, 2, hidden_own)
        return lax.dynamic_index_in_dim(parts, which, 2, keepdims=False).reshape(feats, ff_half)

    def scaled(value, gain):
        return (value.astype(F32) * gain).astype(BF16)

    def in_order(own, other):
        return jnp.where(
            core == 0, jnp.concatenate([own, other]), jnp.concatenate([other, own])
        )

    query_scaled, key_scaled, value_scaled = (
        scaled(w, gain_one) for w in (w_query, key_projection, value_projection)
    )
    out_turned = w_out.T

    def attn_part(which):
        return jnp.concatenate(
            [take_half(w, which) for w in (query_scaled, key_scaled, value_scaled, out_turned)],
            axis=1,
        )

    def gather(block):
        return lax.all_gather(block, CHIPS, axis=0, tiled=True)

    attn_block = in_order(attn_part(core), swap(attn_part(1 - core)))
    qkv_cols = q_cols + 2 * kv_cols
    qkv_full = gather(attn_block[:, :qkv_cols])
    out_full = gather(attn_block[:, qkv_cols:])

    gate_scaled, up_scaled = scaled(w_gate, gain_two), scaled(w_up, gain_two)

    def mlp_part(which):
        return jnp.concatenate([ff_part(gate_scaled, which), ff_part(up_scaled, which)], axis=1)

    mlp_block = in_order(mlp_part(core), swap(mlp_part(1 - core)))
    gate_full = gather(mlp_block[:, :ff_half])
    up_full = gather(mlp_block[:, ff_half:])
    down_full = gather(w_down)

    def both(own):
        return jnp.concatenate([own, swap(own)], axis=1)

    def add_partner(part, back=None):
        low = part.reshape(micros, rows_chip, width).astype(BF16)
        mine = swap(low[:, rows_own:])
        theirs = swap(low[:, :rows_own])
        return part + jnp.concatenate([mine, theirs], axis=1).reshape(rows, width).astype(F32)

    def own_sum(part):
        parts = part.reshape(micros, rows_chip, width)
        return parts[:, :rows_own] + swap(parts[:, rows_own:].astype(BF16)).astype(F32)

    def own_rows(value):
        return value.reshape(micros, rows_chip, -1)[:, :rows_own]

    x_pair = both(inputs[:, 0])
    cot_pair = both(cotangent[:, 0]).reshape(rows, width)
    xf = x_pair.reshape(rows, width).astype(F32)

    if n_row == 2:
        row_order = jnp.stack([chip_row, 1 - chip_row])
    else:
        row_order = jnp.arange(n_row)
    halves = jnp.stack([core, 1 - core])
    chip_ids = (halves[:, None] * rows_own + jnp.arange(rows_own)[None, :]).reshape(-1)
    query_ids = chip_row * rows_chip + chip_ids
    key_ids = (row_order[:, None] * rows_chip + chip_ids[None, :]).reshape(-1)
    segments = [layout(cont_lengths[m, 0], query_ids, prompt_rows) for m in range(micros)]
    key_segments = [layout(cont_lengths[m, 0], key_ids, prompt_rows) for m in range(micros)]
    segment_q, position_q = (jnp.stack(v) for v in zip(*segments))
    segment_k, position_k = (jnp.stack(v) for v in zip(*key_segments))
    visible = (
        ((segment_k[:, None, :] == 0) | (segment_k[:, None, :] == segment_q[:, :, None]))
        & (position_k[:, None, :] <= position_q[:, :, None])
    )[:, None, None]
    cosine, sine = rotation(position_q)

    inverse_one = lax.rsqrt(jnp.mean(xf * xf, axis=-1, keepdims=True) + EPSILON)
    act_one = (xf * inverse_one).astype(BF16)
    qkv = dot(act_one, qkv_full, 1, 0).reshape(micros, rows_chip, qkv_cols)
    queries = (
        rotate(
            qkv[..., :q_cols].reshape(micros, rows_chip, q_heads, HEAD_SIZE), cosine, sine
        )
        * scale
    ).astype(BF16)
    keys_own = (
        rotate(
            qkv[..., q_cols : q_cols + kv_cols].reshape(micros, rows_chip, kv_heads, HEAD_SIZE),
            cosine,
            sine,
        )
        .astype(BF16)
        .reshape(micros, rows_chip, kv_cols)
    )
    values_own = qkv[..., q_cols + kv_cols :].astype(BF16)
    key_value = jnp.concatenate([keys_own, values_own], axis=2)
    flip = [(0, 1), (1, 0)]
    if n_row == 2:
        key_value = jnp.concatenate([key_value, lax.ppermute(key_value, "row", flip)], axis=1)
    else:
        key_value = lax.all_gather(key_value, "row", axis=1, tiled=True)
    keys_all = key_value[..., :kv_cols].reshape(micros, rows_group, kv_heads, HEAD_SIZE)
    values_all = key_value[..., kv_cols:].reshape(micros, rows_group, kv_heads, HEAD_SIZE)
    grouped = queries.reshape(micros, rows_chip, kv_heads, repeat, HEAD_SIZE)

    scores = jnp.einsum("mrgjd,mkgd->mgjrk", grouped, keys_all, preferred_element_type=F32)
    scores = jnp.where(visible, scores, MASK_FILL)
    top = jnp.max(scores, axis=-1, keepdims=True)
    weights = jnp.exp(scores - top)
    probs = weights / jnp.sum(weights, axis=-1, keepdims=True)
    probs_low = probs.astype(BF16)
    attn = jnp.einsum("mgjrk,mkgd->mrgjd", probs_low, values_all, preferred_element_type=F32)
    attn_low = attn.reshape(rows, q_cols).astype(BF16)

    hidden = xf + add_partner(dot(attn_low, out_full, 1, 1))
    inverse_two = lax.rsqrt(jnp.mean(hidden * hidden, axis=-1, keepdims=True) + EPSILON)
    act_two = (hidden * inverse_two).astype(BF16)
    gate_pre = dot(act_two, gate_full, 1, 0)
    up_pre = dot(act_two, up_full, 1, 0)
    sigmoid_gate = jax.nn.sigmoid(gate_pre)
    silu_gate = gate_pre * sigmoid_gate
    mixed = (silu_gate * up_pre).astype(BF16)

    def scatter(grad):
        return lax.psum_scatter(grad.astype(BF16), CHIPS, scatter_dimension=0, tiled=True)

    grad_down = scatter(dot(mixed, cot_pair, 0, 0)).astype(F32)
    outputs = (own_rows(hidden) + own_sum(dot(mixed, down_full, 1, 0))).astype(BF16)
    grad_mixed = dot(cot_pair, down_full, 1, 1)
    grad_gate_pre = (
        grad_mixed * up_pre * sigmoid_gate * (1.0 + gate_pre * (1.0 - sigmoid_gate))
    ).astype(BF16)
    grad_up_pre = (grad_mixed * silu_gate).astype(BF16)
    grad_gate_half = scatter(dot(act_two, grad_gate_pre, 0, 0))
    grad_up_half = scatter(dot(act_two, grad_up_pre, 0, 0))
    back_two = add_partner(dot(grad_gate_pre, gate_full, 1, 1) + dot(grad_up_pre, up_full, 1, 1))
    grad_hidden = (
        cot_pair.astype(F32)
        + inverse_two * back_two
        - hidden * inverse_two**3 * jnp.mean(back_two * hidden, axis=-1, keepdims=True)
    )
    hidden_low = grad_hidden.astype(BF16)
    grad_out_half = scatter(dot(hidden_low, attn_low, 0, 0))
    attn_grad = (
        dot(hidden_low, out_full, 1, 0)
        .astype(BF16)
        .reshape(micros, rows_chip, kv_heads, repeat, HEAD_SIZE)
    )
    grad_probs = jnp.einsum("mrgjd,mkgd->mgjrk", attn_grad, values_all, preferred_element_type=F32)
    delta = jnp.sum(probs * grad_probs, axis=-1, keepdims=True)
    grad_scores = (probs * (grad_probs - delta)).astype(BF16)
    grad_queries = jnp.einsum(
        "mgjrk,mkgd->mrgjd", grad_scores, keys_all, preferred_element_type=F32
    )
    grad_keys = jnp.einsum("mgjrk,mrgjd->mkgd", grad_scores, grouped, preferred_element_type=F32)
    grad_values = jnp.einsum("mgjrk,mrgjd->mkgd", probs_low, attn_grad, preferred_element_type=F32)
    grad_kv = jnp.concatenate(
        [
            grad_keys.reshape(micros, rows_group, kv_cols),
            grad_values.reshape(micros, rows_group, kv_cols),
        ],
        axis=2,
    )
    if n_row == 2:
        grad_kv = grad_kv[:, :rows_chip] + lax.ppermute(
            grad_kv[:, rows_chip:].astype(BF16), "row", flip
        ).astype(F32)
    else:
        grad_kv = lax.psum_scatter(
            grad_kv.astype(BF16), "row", scatter_dimension=1, tiled=True
        ).astype(F32)
    grad_query_pre = rotate(
        grad_queries.reshape(micros, rows_chip, q_heads, HEAD_SIZE) * scale, cosine, -sine
    ).reshape(micros, rows_chip, q_cols)
    grad_key_pre = rotate(
        grad_kv[..., :kv_cols].reshape(micros, rows_chip, kv_heads, HEAD_SIZE), cosine, -sine
    ).reshape(micros, rows_chip, kv_cols)
    grad_qkv_pre = (
        jnp.concatenate([grad_query_pre, grad_key_pre, grad_kv[..., kv_cols:]], axis=2)
        .astype(BF16)
        .reshape(rows, qkv_cols)
    )
    grad_qkv_half = scatter(dot(act_one, grad_qkv_pre, 0, 0))
    back_one = own_sum(dot(grad_qkv_pre, qkv_full, 1, 1))
    x_own = inputs[:, 0].astype(F32)
    inverse_own = own_rows(inverse_one)
    grad_inputs = (
        own_rows(grad_hidden)
        + inverse_own * back_one
        - x_own * inverse_own**3 * jnp.mean(back_one * x_own, axis=-1, keepdims=True)
    )

    def regroup(half):
        own = lax.dynamic_slice_in_dim(half, core * feats, feats, 0)
        other = swap(lax.dynamic_slice_in_dim(half, (1 - core) * feats, feats, 0))
        return own.astype(F32), other.astype(F32)

    def join_columns(own, other):
        return jnp.where(
            core == 0,
            jnp.concatenate([own, other], axis=1),
            jnp.concatenate([other, own], axis=1),
        )

    def join_ff(pair):
        own, other = (part.reshape(feats, chips, 1, hidden_own) for part in pair)
        return jnp.where(
            core == 0,
            jnp.concatenate([own, other], axis=2),
            jnp.concatenate([other, own], axis=2),
        ).reshape(feats, 2 * ff_half)

    bare_gate, bare_up = join_ff(regroup(grad_gate_half)), join_ff(regroup(grad_up_half))
    grad_mlp_gain = jnp.sum(
        bare_gate * w_gate.astype(F32) + bare_up * w_up.astype(F32), axis=1
    )
    own, other = regroup(grad_qkv_half)
    bare_query, bare_key, bare_value = (
        join_columns(own[:, a:b], other[:, a:b])
        for a, b in ((0, q_cols), (q_cols, q_cols + kv_cols), (q_cols + kv_cols, qkv_cols))
    )
    grad_attn_gain = jnp.sum(bare_query * w_query.astype(F32), axis=1) + jnp.sum(
        bare_key * key_projection.astype(F32) + bare_value * value_projection.astype(F32), axis=1
    )
    grad_out = join_columns(*regroup(grad_out_half)).T
    return (
        outputs[:, None],
        grad_inputs[:, None],
        bare_query * gain_one,
        bare_key * gain_one,
        bare_value * gain_one,
        grad_out,
        grad_attn_gain,
        bare_gate * gain_two,
        bare_up * gain_two,
        grad_down,
        grad_mlp_gain,
    )


def solution(mesh):
    grp, seq = mesh.shape["grp"], mesh.shape["seq"]
    split = Mesh(mesh.devices.reshape(grp, seq // 2, 2), ("grp", "row", "core"))
    every = ("grp", "row", "core")
    rows = P(None, "grp", ("row", "core"), None)
    sharded, column = P(every, None), P(None, every)
    return jax.shard_map(
        on_device,
        mesh=split,
        in_specs=(
            rows,
            P(None, "grp", None),
            sharded,
            sharded,
            sharded,
            column,
            P(every),
            sharded,
            sharded,
            sharded,
            P(every),
            rows,
        ),
        out_specs=(
            rows,
            rows,
            sharded,
            sharded,
            sharded,
            column,
            P(every),
            sharded,
            sharded,
            sharded,
            P(every),
        ),
        check_vma=False,
    )
```

```python
import jax
import jax.numpy as jnp
from jax import lax
from jax.sharding import Mesh
from jax.sharding import PartitionSpec as P

QUERY_HEADS = 16
KEY_VALUE_HEADS = 8
HEAD_SIZE = 96
CONT_MEAN = 224

EPSILON = 1e-05
ROPE_BASE = 100000.0
MASK_FILL = -1e30
CHIPS = ("grp", "row")
F32 = jnp.float32
BF16 = jnp.bfloat16


def layout(lengths, row_ids, prompt_rows):
    cont_ends = prompt_rows + jnp.cumsum(lengths)
    cont_starts = cont_ends - lengths
    member = (
        (row_ids[:, None] >= cont_starts[None, :]) & (row_ids[:, None] < cont_ends[None, :])
    ).astype(jnp.int32)
    labels = jnp.arange(1, lengths.shape[0] + 1, dtype=jnp.int32)
    segment = jnp.sum(member * labels[None, :], axis=1)
    offsets = jnp.sum(member * cont_starts[None, :], axis=1)
    position = jnp.where(segment > 0, prompt_rows + row_ids - offsets, row_ids)
    return (segment, position)


def rotation(position):
    half_dim = HEAD_SIZE // 2
    frequency = ROPE_BASE ** (-2.0 * jnp.arange(half_dim, dtype=F32) / HEAD_SIZE)
    angles = position.astype(F32)[..., None] * frequency
    return (jnp.cos(angles)[..., None, :], jnp.sin(angles)[..., None, :])


def rotate(head_values, cosine, sine):
    half_dim = HEAD_SIZE // 2
    first, second = head_values[..., :half_dim], head_values[..., half_dim:]
    return jnp.concatenate(
        [first * cosine - second * sine, second * cosine + first * sine], axis=-1
    )


def dot(left, right, left_dim, right_dim):
    return lax.dot_general(
        left, right, (((left_dim,), (right_dim,)), ((), ())), preferred_element_type=F32
    )


def swap(value):
    return lax.ppermute(value, "core", [(0, 1), (1, 0)])


def take_half(value, which):
    half = value.shape[1] // 2
    return lax.dynamic_slice_in_dim(value, which * half, half, 1)


def on_device_wide(
    inputs,
    cont_lengths,
    w_query,
    key_projection,
    value_projection,
    w_out,
    attn_gain,
    w_gate,
    w_up,
    w_down,
    mlp_gain,
    cotangent,
):
    micros, _, rows_own, width = inputs.shape
    n_row = lax.axis_size("row")
    chips = lax.axis_size("grp") * n_row
    core = lax.axis_index("core")
    chip_row = lax.axis_index("row")
    rows_chip = 2 * rows_own
    rows_group = rows_chip * n_row
    rows = micros * rows_chip
    prompt_rows = rows_group - CONT_MEAN * cont_lengths.shape[2]
    repeat = QUERY_HEADS // KEY_VALUE_HEADS
    kv_heads = KEY_VALUE_HEADS // 2
    q_heads = QUERY_HEADS // 2
    q_cols, kv_cols = q_heads * HEAD_SIZE, kv_heads * HEAD_SIZE
    scale = HEAD_SIZE ** (-0.5)
    feats = w_query.shape[0]
    hidden_own = w_down.shape[0]
    ff_half = hidden_own * chips

    gain_one = attn_gain.astype(F32)[:, None]
    gain_two = mlp_gain.astype(F32)[:, None]

    def ff_part(value, which):
        parts = value.reshape(feats, chips, 2, hidden_own)
        return lax.dynamic_index_in_dim(parts, which, 2, keepdims=False).reshape(feats, ff_half)

    def scaled(value, gain):
        return (value.astype(F32) * gain).astype(BF16)

    def in_order(own, other):
        return jnp.where(
            core == 0, jnp.concatenate([own, other]), jnp.concatenate([other, own])
        )

    query_scaled, key_scaled, value_scaled = (
        scaled(w, gain_one) for w in (w_query, key_projection, value_projection)
    )
    out_turned = w_out.T

    def attn_part(which):
        return jnp.concatenate(
            [take_half(w, which) for w in (query_scaled, key_scaled, value_scaled, out_turned)],
            axis=1,
        )

    def gather(block):
        return lax.all_gather(block, CHIPS, axis=0, tiled=True)

    attn_block = in_order(attn_part(core), swap(attn_part(1 - core)))
    qkv_cols = q_cols + 2 * kv_cols
    qkv_full = gather(attn_block[:, :qkv_cols])
    out_full = gather(attn_block[:, qkv_cols:])

    gate_scaled, up_scaled = scaled(w_gate, gain_two), scaled(w_up, gain_two)

    def mlp_part(which):
        return jnp.concatenate([ff_part(gate_scaled, which), ff_part(up_scaled, which)], axis=1)

    mlp_block = in_order(mlp_part(core), swap(mlp_part(1 - core)))
    gate_full = gather(mlp_block[:, :ff_half])
    up_full = gather(mlp_block[:, ff_half:])
    down_full = gather(w_down)

    def both(own):
        return jnp.concatenate([own, swap(own)], axis=1)

    def add_partner(part, back=None):
        low = part.reshape(micros, rows_chip, width).astype(BF16)
        mine = swap(low[:, rows_own:])
        theirs = swap(low[:, :rows_own])
        return part + jnp.concatenate([mine, theirs], axis=1).reshape(rows, width).astype(F32)

    def own_sum(part):
        parts = part.reshape(micros, rows_chip, width)
        return parts[:, :rows_own] + swap(parts[:, rows_own:].astype(BF16)).astype(F32)

    def own_rows(value):
        return value.reshape(micros, rows_chip, -1)[:, :rows_own]

    x_pair = both(inputs[:, 0])
    cot_pair = both(cotangent[:, 0]).reshape(rows, width)
    xf = x_pair.reshape(rows, width).astype(F32)

    if n_row == 2:
        row_order = jnp.stack([chip_row, 1 - chip_row])
    else:
        row_order = jnp.arange(n_row)
    halves = jnp.stack([core, 1 - core])
    chip_ids = (halves[:, None] * rows_own + jnp.arange(rows_own)[None, :]).reshape(-1)
    query_ids = chip_row * rows_chip + chip_ids
    key_ids = (row_order[:, None] * rows_chip + chip_ids[None, :]).reshape(-1)
    segments = [layout(cont_lengths[m, 0], query_ids, prompt_rows) for m in range(micros)]
    key_segments = [layout(cont_lengths[m, 0], key_ids, prompt_rows) for m in range(micros)]
    segment_q, position_q = (jnp.stack(v) for v in zip(*segments))
    segment_k, position_k = (jnp.stack(v) for v in zip(*key_segments))
    visible = (
        ((segment_k[:, None, :] == 0) | (segment_k[:, None, :] == segment_q[:, :, None]))
        & (position_k[:, None, :] <= position_q[:, :, None])
    )[:, None, None]
    cosine, sine = rotation(position_q)

    inverse_one = lax.rsqrt(jnp.mean(xf * xf, axis=-1, keepdims=True) + EPSILON)
    act_one = (xf * inverse_one).astype(BF16)
    qkv = dot(act_one, qkv_full, 1, 0).reshape(micros, rows_chip, qkv_cols)
    queries = (
        rotate(
            qkv[..., :q_cols].reshape(micros, rows_chip, q_heads, HEAD_SIZE), cosine, sine
        )
        * scale
    ).astype(BF16)
    keys_own = (
        rotate(
            qkv[..., q_cols : q_cols + kv_cols].reshape(micros, rows_chip, kv_heads, HEAD_SIZE),
            cosine,
            sine,
        )
        .astype(BF16)
        .reshape(micros, rows_chip, kv_cols)
    )
    values_own = qkv[..., q_cols + kv_cols :].astype(BF16)
    key_value = jnp.concatenate([keys_own, values_own], axis=2)
    flip = [(0, 1), (1, 0)]
    if n_row == 2:
        key_value = jnp.concatenate([key_value, lax.ppermute(key_value, "row", flip)], axis=1)
    else:
        key_value = lax.all_gather(key_value, "row", axis=1, tiled=True)
    keys_all = key_value[..., :kv_cols].reshape(micros, rows_group, kv_heads, HEAD_SIZE)
    values_all = key_value[..., kv_cols:].reshape(micros, rows_group, kv_heads, HEAD_SIZE)
    grouped = queries.reshape(micros, rows_chip, kv_heads, repeat, HEAD_SIZE)

    scores = jnp.einsum("mrgjd,mkgd->mgjrk", grouped, keys_all, preferred_element_type=F32)
    scores = jnp.where(visible, scores, MASK_FILL)
    top = jnp.max(scores, axis=-1, keepdims=True)
    weights = jnp.exp(scores - top)
    probs = weights / jnp.sum(weights, axis=-1, keepdims=True)
    probs_low = probs.astype(BF16)
    attn = jnp.einsum("mgjrk,mkgd->mrgjd", probs_low, values_all, preferred_element_type=F32)
    attn_low = attn.reshape(rows, q_cols).astype(BF16)

    hidden = xf + add_partner(dot(attn_low, out_full, 1, 1))
    inverse_two = lax.rsqrt(jnp.mean(hidden * hidden, axis=-1, keepdims=True) + EPSILON)
    act_two = (hidden * inverse_two).astype(BF16)
    gate_pre = dot(act_two, gate_full, 1, 0)
    up_pre = dot(act_two, up_full, 1, 0)
    sigmoid_gate = jax.nn.sigmoid(gate_pre)
    silu_gate = gate_pre * sigmoid_gate
    mixed = (silu_gate * up_pre).astype(BF16)

    def scatter(grad):
        return lax.psum_scatter(grad.astype(BF16), CHIPS, scatter_dimension=0, tiled=True)

    grad_down = scatter(dot(mixed, cot_pair, 0, 0)).astype(F32)
    outputs = (own_rows(hidden) + own_sum(dot(mixed, down_full, 1, 0))).astype(BF16)
    grad_mixed = dot(cot_pair, down_full, 1, 1)
    grad_gate_pre = (
        grad_mixed * up_pre * sigmoid_gate * (1.0 + gate_pre * (1.0 - sigmoid_gate))
    ).astype(BF16)
    grad_up_pre = (grad_mixed * silu_gate).astype(BF16)
    grad_gate_half = scatter(dot(act_two, grad_gate_pre, 0, 0))
    grad_up_half = scatter(dot(act_two, grad_up_pre, 0, 0))
    back_two = add_partner(dot(grad_gate_pre, gate_full, 1, 1) + dot(grad_up_pre, up_full, 1, 1))
    grad_hidden = (
        cot_pair.astype(F32)
        + inverse_two * back_two
        - hidden * inverse_two**3 * jnp.mean(back_two * hidden, axis=-1, keepdims=True)
    )
    hidden_low = grad_hidden.astype(BF16)
    grad_out_half = scatter(dot(hidden_low, attn_low, 0, 0))
    attn_grad = (
        dot(hidden_low, out_full, 1, 0)
        .astype(BF16)
        .reshape(micros, rows_chip, kv_heads, repeat, HEAD_SIZE)
    )
    grad_probs = jnp.einsum("mrgjd,mkgd->mgjrk", attn_grad, values_all, preferred_element_type=F32)
    delta = jnp.sum(probs * grad_probs, axis=-1, keepdims=True)
    grad_scores = (probs * (grad_probs - delta)).astype(BF16)
    grad_queries = jnp.einsum(
        "mgjrk,mkgd->mrgjd", grad_scores, keys_all, preferred_element_type=F32
    )
    grad_keys = jnp.einsum("mgjrk,mrgjd->mkgd", grad_scores, grouped, preferred_element_type=F32)
    grad_values = jnp.einsum("mgjrk,mrgjd->mkgd", probs_low, attn_grad, preferred_element_type=F32)
    grad_kv = jnp.concatenate(
        [
            grad_keys.reshape(micros, rows_group, kv_cols),
            grad_values.reshape(micros, rows_group, kv_cols),
        ],
        axis=2,
    )
    if n_row == 2:
        grad_kv = grad_kv[:, :rows_chip] + lax.ppermute(
            grad_kv[:, rows_chip:].astype(BF16), "row", flip
        ).astype(F32)
    else:
        grad_kv = lax.psum_scatter(
            grad_kv.astype(BF16), "row", scatter_dimension=1, tiled=True
        ).astype(F32)
    grad_query_pre = rotate(
        grad_queries.reshape(micros, rows_chip, q_heads, HEAD_SIZE) * scale, cosine, -sine
    ).reshape(micros, rows_chip, q_cols)
    grad_key_pre = rotate(
        grad_kv[..., :kv_cols].reshape(micros, rows_chip, kv_heads, HEAD_SIZE), cosine, -sine
    ).reshape(micros, rows_chip, kv_cols)
    grad_qkv_pre = (
        jnp.concatenate([grad_query_pre, grad_key_pre, grad_kv[..., kv_cols:]], axis=2)
        .astype(BF16)
        .reshape(rows, qkv_cols)
    )
    grad_qkv_half = scatter(dot(act_one, grad_qkv_pre, 0, 0))
    back_one = own_sum(dot(grad_qkv_pre, qkv_full, 1, 1))
    x_own = inputs[:, 0].astype(F32)
    inverse_own = own_rows(inverse_one)
    grad_inputs = (
        own_rows(grad_hidden)
        + inverse_own * back_one
        - x_own * inverse_own**3 * jnp.mean(back_one * x_own, axis=-1, keepdims=True)
    )

    def regroup(half):
        own = lax.dynamic_slice_in_dim(half, core * feats, feats, 0)
        other = swap(lax.dynamic_slice_in_dim(half, (1 - core) * feats, feats, 0))
        return own.astype(F32), other.astype(F32)

    def join_columns(own, other):
        return jnp.where(
            core == 0,
            jnp.concatenate([own, other], axis=1),
            jnp.concatenate([other, own], axis=1),
        )

    def join_ff(pair):
        own, other = (part.reshape(feats, chips, 1, hidden_own) for part in pair)
        return jnp.where(
            core == 0,
            jnp.concatenate([own, other], axis=2),
            jnp.concatenate([other, own], axis=2),
        ).reshape(feats, 2 * ff_half)

    bare_gate, bare_up = join_ff(regroup(grad_gate_half)), join_ff(regroup(grad_up_half))
    grad_mlp_gain = jnp.sum(
        bare_gate * w_gate.astype(F32) + bare_up * w_up.astype(F32), axis=1
    )
    own, other = regroup(grad_qkv_half)
    bare_query, bare_key, bare_value = (
        join_columns(own[:, a:b], other[:, a:b])
        for a, b in ((0, q_cols), (q_cols, q_cols + kv_cols), (q_cols + kv_cols, qkv_cols))
    )
    grad_attn_gain = jnp.sum(bare_query * w_query.astype(F32), axis=1) + jnp.sum(
        bare_key * key_projection.astype(F32) + bare_value * value_projection.astype(F32), axis=1
    )
    grad_out = join_columns(*regroup(grad_out_half)).T
    return (
        outputs[:, None],
        grad_inputs[:, None],
        bare_query * gain_one,
        bare_key * gain_one,
        bare_value * gain_one,
        grad_out,
        grad_attn_gain,
        bare_gate * gain_two,
        bare_up * gain_two,
        grad_down,
        grad_mlp_gain,
    )


def pair_flip(value, axis):
    return lax.ppermute(value, axis, [(0, 1), (1, 0)])


def line_pairs(senders, step, fold):
    return [(z * 2 + x, (z + step) * 2 + (1 - x if fold else x)) for z in senders for x in (0, 1)]


def shift(value, senders, step):
    return lax.ppermute(value, ("z", "x"), line_pairs(senders, step, False))


def cross(value, holders):
    return lax.ppermute(value, ("z", "x"), line_pairs(holders, 0, True))


def gather_blocks(block):
    depth = lax.axis_size("z")
    z, x = lax.axis_index("z"), lax.axis_index("x")
    zero = jnp.zeros((), jnp.int32)
    whole = jnp.zeros((3 * depth - 2, 2) + block.shape, block.dtype)

    def put(whole, value, offset, side):
        return lax.dynamic_update_slice(
            whole, value[None, None], (z + depth - 1 + offset, side, zero, zero)
        )

    up = down = block
    pieces = [(block, 0, x), (cross(block, range(depth)), 0, 1 - x)]
    for step in range(1, depth):
        up = shift(up, range(step - 1, depth - 1), 1)
        down = shift(down, range(1, depth - step + 1), -1)
        pieces += [
            (up, -step, x),
            (down, step, x),
            (cross(up, range(step, depth)), -step, 1 - x),
            (cross(down, range(0, depth - step)), step, 1 - x),
        ]
    for value, offset, side in pieces:
        whole = put(whole, value, offset, side)
    return whole[depth - 1 : 2 * depth - 1].reshape(2 * depth * block.shape[0], block.shape[1])


def reduce_blocks(grad):
    depth = lax.axis_size("z")
    z, x = lax.axis_index("z"), lax.axis_index("x")
    zero = jnp.zeros((), jnp.int32)
    rows, cols = grad.shape[0] // (2 * depth), grad.shape[1]
    parts = grad.reshape(depth, 2, rows, cols)

    def local(offset, side):
        at = jnp.clip(z + offset, 0, depth - 1)
        return lax.dynamic_slice(parts, (at, side, zero, zero), (1, 1, rows, cols))[0, 0]

    def both_sides(offset):
        holders = [at for at in range(depth) if 0 <= at + offset < depth]
        other = cross(local(offset, 1 - x).astype(BF16), holders)
        return local(offset, x).astype(F32) + other.astype(F32)

    up = down = None
    for step in range(1, depth):
        sum_up, sum_down = both_sides(depth - step), both_sides(step - depth)
        if step > 1:
            sum_up, sum_down = sum_up + up.astype(F32), sum_down + down.astype(F32)
        up = shift(sum_up.astype(BF16), range(0, step), 1)
        down = shift(sum_down.astype(BF16), range(depth - step, depth), -1)
    return both_sides(0) + up.astype(F32) + down.astype(F32)


def on_device(
    inputs,
    cont_lengths,
    w_query,
    key_projection,
    value_projection,
    w_out,
    attn_gain,
    w_gate,
    w_up,
    w_down,
    mlp_gain,
    cotangent,
):
    micros, _, rows_own, width = inputs.shape
    chips = lax.axis_size("z") * lax.axis_size("x")
    core, y = lax.axis_index("core"), lax.axis_index("y")
    set_rows = micros * rows_own
    rows = 4 * set_rows
    rows_group = 4 * rows_own
    prompt_rows = rows_group - CONT_MEAN * cont_lengths.shape[2]
    repeat = QUERY_HEADS // KEY_VALUE_HEADS
    q_heads, kv_heads = QUERY_HEADS // 4, KEY_VALUE_HEADS // 4
    q_cols, kv_cols = q_heads * HEAD_SIZE, kv_heads * HEAD_SIZE
    qkv_cols = q_cols + 2 * kv_cols
    scale = HEAD_SIZE ** (-0.5)
    feats = w_query.shape[0]
    hidden_own = w_down.shape[0]
    ff_cols = hidden_own * chips
    gain_one = attn_gain.astype(F32)[:, None]
    gain_two = mlp_gain.astype(F32)[:, None]

    def scaled(value, gain):
        return (value.astype(F32) * gain).astype(BF16)

    def natural(mine, over_y, over_core, over_both):
        near = jnp.where(core == 0, jnp.stack([mine, over_core]), jnp.stack([over_core, mine]))
        far = jnp.where(
            core == 0, jnp.stack([over_y, over_both]), jnp.stack([over_both, over_y])
        )
        return jnp.where(y == 0, jnp.concatenate([near, far]), jnp.concatenate([far, near]))

    mine_id = y * 2 + core
    y_id = (1 - y) * 2 + core
    core_id = y * 2 + 1 - core
    both_id = (1 - y) * 2 + 1 - core

    def columns(value, which, size):
        return lax.dynamic_slice_in_dim(value, which * size, size, 1)

    def ff_part(value, which):
        parts = value.reshape(feats, chips, 4, hidden_own)
        return lax.dynamic_index_in_dim(parts, which, 2, keepdims=False).reshape(feats, ff_cols)

    def spread(part_of):
        own_part = part_of(mine_id)
        cols = own_part.shape[1]
        over_y = pair_flip(jnp.concatenate([part_of(y_id), part_of(both_id)], axis=1), "y")
        over_core = pair_flip(
            jnp.concatenate([part_of(core_id), over_y[:, cols:]], axis=0), "core"
        )
        return natural(
            own_part, over_y[:, :cols], over_core[:feats], over_core[feats:]
        ).reshape(4 * feats, cols)

    def collect(quarter):
        def rows_of(which):
            return lax.dynamic_slice_in_dim(quarter, which * feats, feats, 0)

        cols = quarter.shape[1]
        from_core = pair_flip(
            jnp.concatenate([rows_of(core_id), rows_of(both_id)]).astype(BF16), "core"
        )
        over_y = pair_flip(
            jnp.concatenate([rows_of(y_id).astype(BF16), from_core[feats:]], axis=1), "y"
        )
        return natural(
            rows_of(mine_id),
            over_y[:, :cols].astype(F32),
            from_core[:feats].astype(F32),
            over_y[:, cols:].astype(F32),
        )

    query_scaled, key_scaled, value_scaled = (
        scaled(w, gain_one) for w in (w_query, key_projection, value_projection)
    )
    out_turned = w_out.T
    gate_scaled, up_scaled = scaled(w_gate, gain_two), scaled(w_up, gain_two)

    def attn_part(which):
        return jnp.concatenate(
            [
                columns(query_scaled, which, q_cols),
                columns(key_scaled, which, kv_cols),
                columns(value_scaled, which, kv_cols),
                columns(out_turned, which, q_cols),
            ],
            axis=1,
        )

    def mlp_part(which):
        return jnp.concatenate([ff_part(gate_scaled, which), ff_part(up_scaled, which)], axis=1)

    attn_full = gather_blocks(spread(attn_part))
    qkv_full, out_full = attn_full[:, :qkv_cols], attn_full[:, qkv_cols:]
    gate_up_full = gather_blocks(spread(mlp_part))
    down_full = gather_blocks(w_down)

    def share(own):
        over_y = pair_flip(own, "y")
        over_core = pair_flip(own, "core")
        over_both = pair_flip(over_y, "core")
        return jnp.concatenate([own, over_y, over_core, over_both])

    def own_sum(part):
        low = part[2 * set_rows :].astype(BF16)
        near = part[: 2 * set_rows] + pair_flip(low, "core").astype(F32)
        return near[:set_rows] + pair_flip(near[set_rows:].astype(BF16), "y").astype(F32)

    x_own = inputs.reshape(set_rows, width)
    cot_own = cotangent.reshape(set_rows, width)
    xf = x_own.astype(F32)
    inverse_one = lax.rsqrt(jnp.mean(xf * xf, axis=-1, keepdims=True) + EPSILON)
    act_one = share((xf * inverse_one).astype(BF16))
    cot_all = share(cot_own)

    sets = jnp.stack([mine_id, y_id, core_id, both_id])
    row_ids = (sets[:, None] * rows_own + jnp.arange(rows_own)[None, :]).reshape(-1)
    segment, position = (
        jnp.stack(v)
        for v in zip(*[layout(cont_lengths[m, 0], row_ids, prompt_rows) for m in range(micros)])
    )
    visible = (
        ((segment[:, None, :] == 0) | (segment[:, None, :] == segment[:, :, None]))
        & (position[:, None, :] <= position[:, :, None])
    )[:, None, None]
    cosine, sine = rotation(position)

    def by_micro(value, heads):
        return (
            value.reshape(4, micros, rows_own, heads, HEAD_SIZE)
            .transpose(1, 0, 2, 3, 4)
            .reshape(micros, rows_group, heads, HEAD_SIZE)
        )

    def by_set(value):
        return (
            value.reshape(micros, 4, rows_own, -1).transpose(1, 0, 2, 3).reshape(rows, -1)
        )

    qkv = dot(act_one, qkv_full, 1, 0)
    queries = (
        (rotate(by_micro(qkv[:, :q_cols], q_heads), cosine, sine) * scale)
        .astype(BF16)
        .reshape(micros, rows_group, kv_heads, repeat, HEAD_SIZE)
    )
    keys = rotate(by_micro(qkv[:, q_cols : q_cols + kv_cols], kv_heads), cosine, sine).astype(BF16)
    values = by_micro(qkv[:, q_cols + kv_cols :], kv_heads).astype(BF16)
    scores = jnp.einsum("mrgjd,mkgd->mgjrk", queries, keys, preferred_element_type=F32)
    scores = jnp.where(visible, scores, MASK_FILL)
    top = jnp.max(scores, axis=-1, keepdims=True)
    weights = jnp.exp(scores - top)
    probs = weights / jnp.sum(weights, axis=-1, keepdims=True)
    probs_low = probs.astype(BF16)
    attn = jnp.einsum("mgjrk,mkgd->mrgjd", probs_low, values, preferred_element_type=F32)
    attn_low = by_set(attn.astype(BF16))

    hidden = xf + own_sum(dot(attn_low, out_full, 1, 1))
    inverse_two = lax.rsqrt(jnp.mean(hidden * hidden, axis=-1, keepdims=True) + EPSILON)
    act_two = share((hidden * inverse_two).astype(BF16))
    gate_pre = dot(act_two, gate_up_full[:, :ff_cols], 1, 0)
    up_pre = dot(act_two, gate_up_full[:, ff_cols:], 1, 0)
    sigmoid_gate = jax.nn.sigmoid(gate_pre)
    silu_gate = gate_pre * sigmoid_gate
    mixed = (silu_gate * up_pre).astype(BF16)

    grad_down = reduce_blocks(dot(mixed, cot_all, 0, 0).astype(BF16))
    outputs = (hidden + own_sum(dot(mixed, down_full, 1, 0))).astype(BF16)
    grad_mixed = dot(cot_all, down_full, 1, 1)
    grad_gate_pre = (
        grad_mixed * up_pre * sigmoid_gate * (1.0 + gate_pre * (1.0 - sigmoid_gate))
    ).astype(BF16)
    grad_up_pre = (grad_mixed * silu_gate).astype(BF16)
    grad_gate_up_pre = jnp.concatenate([grad_gate_pre, grad_up_pre], axis=1)
    gate_up_quarter = reduce_blocks(dot(act_two, grad_gate_up_pre, 0, 0).astype(BF16))
    back_two = own_sum(dot(grad_gate_up_pre, gate_up_full, 1, 1))
    grad_hidden = (
        cot_own.astype(F32)
        + inverse_two * back_two
        - hidden * inverse_two**3 * jnp.mean(back_two * hidden, axis=-1, keepdims=True)
    )
    hidden_low = share(grad_hidden.astype(BF16))
    out_quarter = reduce_blocks(dot(hidden_low, attn_low, 0, 0).astype(BF16))
    attn_grad = by_micro(dot(hidden_low, out_full, 1, 0).astype(BF16), q_heads).reshape(
        micros, rows_group, kv_heads, repeat, HEAD_SIZE
    )
    grad_probs = jnp.einsum("mrgjd,mkgd->mgjrk", attn_grad, values, preferred_element_type=F32)
    delta = jnp.sum(probs * grad_probs, axis=-1, keepdims=True)
    grad_scores = (probs * (grad_probs - delta)).astype(BF16)
    grad_queries = jnp.einsum("mgjrk,mkgd->mrgjd", grad_scores, keys, preferred_element_type=F32)
    grad_keys = jnp.einsum("mgjrk,mrgjd->mkgd", grad_scores, queries, preferred_element_type=F32)
    grad_values = jnp.einsum("mgjrk,mrgjd->mkgd", probs_low, attn_grad, preferred_element_type=F32)
    grad_queries = grad_queries.reshape(micros, rows_group, q_heads, HEAD_SIZE)
    grad_qkv_pre = jnp.concatenate(
        [
            by_set(rotate(grad_queries * scale, cosine, -sine).astype(BF16)),
            by_set(rotate(grad_keys, cosine, -sine).astype(BF16)),
            by_set(grad_values.astype(BF16)),
        ],
        axis=1,
    )
    qkv_quarter = reduce_blocks(dot(act_one, grad_qkv_pre, 0, 0).astype(BF16))
    back_one = own_sum(dot(grad_qkv_pre, qkv_full, 1, 1))
    grad_inputs = (
        grad_hidden
        + inverse_one * back_one
        - xf * inverse_one**3 * jnp.mean(back_one * xf, axis=-1, keepdims=True)
    )

    def side_by_side(parts):
        return parts.transpose(1, 0, 2).reshape(feats, -1)

    def ff_join(parts):
        return (
            parts.reshape(4, feats, chips, hidden_own)
            .transpose(1, 2, 0, 3)
            .reshape(feats, 4 * ff_cols)
        )

    gate_up_parts = collect(gate_up_quarter)
    bare_gate, bare_up = ff_join(gate_up_parts[..., :ff_cols]), ff_join(gate_up_parts[..., ff_cols:])
    grad_mlp_gain = jnp.sum(bare_gate * w_gate.astype(F32) + bare_up * w_up.astype(F32), axis=1)
    grad_out = side_by_side(collect(out_quarter)).T
    qkv_parts = collect(qkv_quarter)
    bare_query = side_by_side(qkv_parts[..., :q_cols])
    bare_key = side_by_side(qkv_parts[..., q_cols : q_cols + kv_cols])
    bare_value = side_by_side(qkv_parts[..., q_cols + kv_cols :])
    grad_attn_gain = jnp.sum(bare_query * w_query.astype(F32), axis=1) + jnp.sum(
        bare_key * key_projection.astype(F32) + bare_value * value_projection.astype(F32), axis=1
    )
    return (
        outputs.reshape(inputs.shape),
        grad_inputs.reshape(inputs.shape),
        bare_query * gain_one,
        bare_key * gain_one,
        bare_value * gain_one,
        grad_out,
        grad_attn_gain,
        bare_gate * gain_two,
        bare_up * gain_two,
        grad_down,
        grad_mlp_gain,
    )


def solution(mesh):
    grp, seq = mesh.shape["grp"], mesh.shape["seq"]
    if seq == 4 and grp % 2 == 0:
        body, outer, inner = on_device, ("z", "x"), ("y", "core")
        split = Mesh(mesh.devices.reshape(grp // 2, 2, 2, 2), outer + inner)
    else:
        body, outer, inner = on_device_wide, ("grp",), ("row", "core")
        split = Mesh(mesh.devices.reshape(grp, seq // 2, 2), outer + inner)
    every = outer + inner
    rows = P(None, outer, inner, None)
    sharded, column, vector = P(every, None), P(None, every), P(every)
    weights = (sharded, sharded, sharded, column, vector, sharded, sharded, sharded, vector)
    return jax.shard_map(
        body,
        mesh=split,
        in_specs=(rows, P(None, outer, None)) + weights + (rows,),
        out_specs=(rows, rows) + weights,
        check_vma=False,
    )
```
